256 devices in a mesh: dp: 128 (over z, y, x), mp: 2 (over core).
Axes of the slice: x: 4, y: 4, z: 8, core: 2. Of those that a mesh axis runs over, the one named last changes fastest.
Arguments:
- points: bfloat16 [131072, 1024], P(('dp', 'mp')), may hold values from -6 to 6
- centroids: bfloat16 [4096, 1024], P('mp'), may hold values from -6 to 6
- assign: int32 [131072], P(('dp', 'mp')), may hold values from 0 to 4095
- keep_mask: int32 [131072], P(('dp', 'mp')), may hold values 0 or 1
Outputs:
- new_centroids: float32 [4096, 1024], P('mp')
- row_cost: float32 [131072], P(('dp', 'mp'))
The draws below stay inside these ranges and needn't reach their ends.
All inputs are finite; a program needn't handle non-finite values. No bound on the sum of `keep_mask` on one device may be relied on, other than what follows from the above.
Results may differ from the reference program's by a relative error of at most 0.0008.
Values may be sent and summed in bfloat16 or wider, within the bound.
No kernel may reach another device: no remote copies, remote signals or barrier semaphores. Data moves between devices by JAX's collectives and lax.ppermute only.
A program may use at most 128 MiB of HBM per device.

```python
import math
import jax
import jax.numpy as jnp
import numpy as np
from jax import lax

D = 1024
K = 4096
ROWS = 131072


def place_ends(values, stream_key, smallest, high):
    longest = values.shape.index(max(values.shape))
    spots = []
    for shift in (0, 1):
        where = [jax.random.randint(jax.random.fold_in(stream_key, axis), (), 0, length) for axis, length in enumerate(values.shape)]
        where[longest] = (where[longest] + shift) % values.shape[longest]
        spots.append(tuple(where))
    return values.at[spots[0]].set(smallest).at[spots[1]].set(high)


def block_scale(own_key, dims, shards, smallest, high):
    level = 1.0
    for axis_at, shards_of in shards:
        draws = jax.random.uniform(jax.random.fold_in(jax.random.fold_in(own_key, 6), axis_at), (shards_of,), jnp.float32, smallest / len(shards), high / len(shards))
        level = level * jnp.repeat(jnp.exp(draws), dims[axis_at] // shards_of).reshape((-1,) + (1,) * (len(dims) - 1 - axis_at))
    return level


def cumulative_ranks(count, lean):
    portions = [(1 << 20) // math.isqrt(standing ** lean) + 1 for standing in range(1, count + 1)]
    width = 1 + sum(portions) // (1 << 30)
    return np.cumsum(np.array([max(1, weight // width) for weight in portions]))


def skewed_ids(own_key, extent, count, skew):
    grid = cumulative_ranks(count, skew)
    pick = jax.random.randint(jax.random.fold_in(own_key, 1), extent, 0, int(grid[count - 1]))
    standing = jnp.searchsorted(jnp.asarray(grid, jnp.int32), pick, side="right")
    return jax.random.permutation(jax.random.fold_in(own_key, 2), count)[standing].astype(jnp.int32)


def centred(own_key, shape, deviation, limit, cuts=(), kind=jnp.bfloat16):
    result = deviation * jax.random.normal(own_key, shape, jnp.float32)
    if cuts:
        result = result * block_scale(own_key, shape, cuts, -0.22, 0.18)
    return jnp.clip(result, -limit, limit).astype(kind)


def setup_inputs(seed: int = 0) -> dict:
    seeds = jax.random.split(jax.random.key(seed), 5)
    points = centred(seeds[0], (ROWS, D), 1.0, 6.0, ((0, 256),))
    centroids = centred(seeds[1], (K, D), 1.0, 6.0, ((0, 2),))
    assign = place_ends(skewed_ids(seeds[2], (ROWS,), K, 2), jax.random.fold_in(seeds[2], 3), 0, K - 1).astype(jnp.int32)
    keep_mask = place_ends((jax.random.randint(seeds[3], (ROWS,), 0, 4) < 3).astype(jnp.int32), jax.random.fold_in(seeds[3], 1), 0, 1)
    return dict(points=points, centroids=centroids, assign=assign, keep_mask=keep_mask)


def reference(points, centroids, assign, keep_mask):
    cent_f = centroids.astype(jnp.float32)
    cent_sq = jnp.sum(cent_f * cent_f, axis=1)
    block = math.gcd(ROWS, 1024)
    blocks = points.reshape(ROWS // block, block, D)

    def cost_block(group_rows):
        point_f = group_rows.astype(jnp.float32)
        point_sq = jnp.sum(point_f * point_f, axis=1)
        inner = jnp.dot(group_rows, centroids.T, preferred_element_type=jnp.float32)
        dist = point_sq[:, None] - 2.0 * inner + cent_sq[None, :]
        return jnp.min(dist, axis=1) / D

    row_cost = lax.map(cost_block, blocks).reshape(ROWS)
    weights = keep_mask.astype(jnp.float32)
    sums = jax.ops.segment_sum(points.astype(jnp.float32) * weights[:, None], assign, num_segments=K)
    counts = jax.ops.segment_sum(weights, assign, num_segments=K)
    fresh = sums / jnp.maximum(counts, 1.0)[:, None]
    new_centroids = jnp.where(counts[:, None] > 0.5, fresh, cent_f)
    return new_centroids, row_cost
```

```python
import jax
import jax.numpy as jnp
from jax import lax
from jax.experimental import pallas as pl
from jax.experimental.pallas import tpu as pltpu
from jax.sharding import Mesh
from jax.sharding import PartitionSpec as P

F32, BF16, I32 = jnp.float32, jnp.bfloat16, jnp.int32
LEVELS = 32767.0


def iota(shape, dim):
    return lax.broadcasted_iota(I32, shape, dim)


def sums_kernel(core_ref, x_ref, own_ref, send_ref):
    step = pl.program_id(0)

    @pl.when(step == 0)
    def _():
        own_ref[...] = jnp.zeros_like(own_ref)
        send_ref[...] = jnp.zeros_like(send_ref)

    core = core_ref[0]
    rows = x_ref.shape[2]
    digits = x_ref[0, 64:80, :].astype(F32)
    code = (digits[0:1] * 64.0 + digits[1:2]).astype(I32)
    low, high = code & 1023, code >> 10
    pick = (iota((1024, rows), 0) == low).astype(BF16)
    pts = x_ref[0, 0:64, :]
    masked = jnp.concatenate(
        [pts * (high == (b ^ (2 * core))).astype(BF16) for b in range(4)], axis=0
    )
    nt = (((1,), (1,)), ((), ()))
    part = lax.dot_general(pick, masked, nt, preferred_element_type=F32)
    own_ref[:, 0:128, :] += part[:, 0:128].reshape(8, 128, 128)
    send_ref[:, 0:128, :] += part[:, 128:256].reshape(8, 128, 128)
    slot = jnp.where(code < 4096, (low & 31) * 4 + high, -1)
    count_rows = (iota((32, rows), 0) == (low >> 5)).astype(BF16)
    count_cols = (iota((128, rows), 0) == slot).astype(BF16)
    counts = lax.dot_general(count_rows, count_cols, nt, preferred_element_type=F32)
    for z in range(8):
        own_ref[z, 128:132, :] += counts[z * 4 : z * 4 + 4]
        send_ref[z, 128:132, :] += counts[z * 4 : z * 4 + 4]


def partial_sums(core, x):
    return pl.pallas_call(
        sums_kernel,
        grid_spec=pltpu.PrefetchScalarGridSpec(
            num_scalar_prefetch=1,
            grid=(x.shape[0],),
            in_specs=[pl.BlockSpec((1, 80, 512), lambda s, c: (s, 0, 0))],
            out_specs=[pl.BlockSpec((8, 136, 128), lambda s, c: (0, 0, 0))] * 2,
        ),
        out_shape=[jax.ShapeDtypeStruct((8, 136, 128), F32)] * 2,
        compiler_params=pltpu.CompilerParams(dimension_semantics=("arbitrary",)),
        name="partial_sums",
    )(core, x)


def mean_kernel(core_ref, t_ref, prior_ref, w_ref):
    total = t_ref[0]
    for z in range(1, 8):
        total = total + t_ref[z]
    sums, counts = total[0:128], total[128:132]
    core = core_ref[0]
    row, lane = iota((128, 128), 0), iota((128, 128), 1)
    wide = jnp.concatenate([jnp.broadcast_to(counts[k : k + 1], (32, 128)) for k in range(4)], 0)
    wide = jnp.where((lane >> 2) == (row & 31), wide, 0.0)
    spread = ((row & 3) == (lane >> 6) + 2 * core).astype(F32)
    count = jnp.dot(wide, spread, precision=lax.Precision.HIGHEST, preferred_element_type=F32)
    mean = jnp.where(count > 0.5, sums / jnp.maximum(count, 1.0), prior_ref[...].astype(F32))
    peak = jnp.max(jnp.abs(mean), axis=0, keepdims=True)
    power = jnp.ceil(jnp.log2(jnp.maximum(peak, 1e-30)))
    q = jnp.round(mean * (LEVELS * jnp.exp2(-power)))
    q = jnp.clip(q, -LEVELS, LEVELS).astype(I32)
    w_ref[0:64, :] = (q[0:64] & 0xFFFF) | (q[64:128] << 16)
    w_ref[64:72, :] = jnp.broadcast_to(power.astype(I32), (8, 128))


def encoded_mean(core, t, prior):
    return pl.pallas_call(
        mean_kernel,
        in_specs=[
            pl.BlockSpec(memory_space=pltpu.SMEM),
            pl.BlockSpec(memory_space=pltpu.VMEM),
            pl.BlockSpec(memory_space=pltpu.VMEM),
        ],
        out_specs=pl.BlockSpec(memory_space=pltpu.VMEM),
        out_shape=jax.ShapeDtypeStruct((72, 128), I32),
        name="encoded_mean",
    )(core, t, prior)


def decode(block):
    packed = block[0:64]
    scale = jnp.exp2(block[64:65].astype(F32)) * (1.0 / LEVELS)
    first = ((packed << 16) >> 16).astype(F32) * scale
    second = (packed >> 16).astype(F32) * scale
    return first, second


def spread_kernel(a_ref, b_ref, out_ref):
    z = pl.program_id(0)
    left = iota((64, 128), 1) < 64

    def fill(block_of):
        for t in range(8):
            even = decode(block_of(2 * t))
            odd = decode(block_of(2 * t + 1))
            for h in range(2):
                e, o = even[h], odd[h]
                rows = slice(h * 64, h * 64 + 64)
                lanes = slice(t * 128, t * 128 + 128)
                out_ref[0, 0, rows, lanes] = jnp.where(left, e, pltpu.roll(o, 64, 1))
                out_ref[1, 0, rows, lanes] = jnp.where(left, pltpu.roll(e, 64, 1), o)

    @pl.when(z < 4)
    def _():
        fill(lambda yx: a_ref[yx % 4, yx // 4, 0])

    @pl.when(z >= 4)
    def _():
        fill(lambda yx: b_ref[yx // 4, yx % 4, 0])


def spread(a, b):
    return pl.pallas_call(
        spread_kernel,
        grid=(8,),
        in_specs=[
            pl.BlockSpec((4, 4, 1, 72, 128), lambda z: (0, 0, jnp.minimum(z, 3), 0, 0)),
            pl.BlockSpec((4, 4, 1, 72, 128), lambda z: (0, 0, jnp.maximum(z - 4, 0), 0, 0)),
        ],
        out_specs=pl.BlockSpec((2, 1, 128, 1024), lambda z: (0, z, 0, 0)),
        out_shape=jax.ShapeDtypeStruct((2, 8, 128, 1024), F32),
        compiler_params=pltpu.CompilerParams(dimension_semantics=("arbitrary",)),
        name="spread",
    )(a, b)


def gather(v, axis):
    size = lax.axis_size(axis)
    return lax.all_to_all(jnp.broadcast_to(v[None], (size,) + v.shape), axis, 0, 0)


def shards(points, centroids, assign, keep_mask):
    width = points.shape[1]
    swap = [(0, 1), (1, 0)]
    core = lax.axis_index("core").astype(I32)[None]
    other = lax.ppermute(centroids, "core", swap)

    code = jnp.where(keep_mask == 1, assign, 4096)
    digits = jnp.stack([code >> 6, code & 63]).astype(BF16)
    digits = jnp.concatenate([digits, jnp.zeros((14, 512), BF16)], axis=0)
    columns = points.T.reshape(16, 64, 512)
    x = jnp.concatenate([columns, jnp.broadcast_to(digits[None], (16, 16, 512))], axis=1)
    x = lax.all_to_all(x, ("y", "x"), 0, 0)

    own, send = partial_sums(core, x)
    t = own + lax.ppermute(send, "core", swap)
    t = lax.all_to_all(t, "z", 0, 0)
    plane = lax.axis_index("y") * 4 + lax.axis_index("x")
    prior = lax.dynamic_slice(
        centroids.reshape(2, 8, 128, width),
        (0, lax.axis_index("z"), 0, plane * 64),
        (2, 1, 128, 64),
    )
    prior = prior.reshape(2, 128, 64).transpose(1, 0, 2).reshape(128, 128)
    w = encoded_mean(core, t, prior)
    w = gather(w, "z")
    a = gather(gather(w[0:4], "y"), "x")
    b = gather(gather(w[4:8], "x"), "y")
    new_centroids = spread(a, b).reshape(2048, width)

    point_f = points.astype(F32)
    point_sq = jnp.sum(point_f * point_f, axis=1)

    def nearest(c):
        inner = lax.dot_general(
            points, c, (((1,), (1,)), ((), ())), preferred_element_type=F32
        )
        c_f = c.astype(F32)
        return jnp.min(jnp.sum(c_f * c_f, axis=1)[None, :] - 2.0 * inner, axis=1)

    row_cost = (point_sq + jnp.minimum(nearest(centroids), nearest(other))) / width
    return new_centroids, row_cost


def solution(mesh):
    grid = Mesh(mesh.devices.reshape(8, 4, 4, 2), ("z", "y", "x", "core"))
    rows = ("z", "y", "x", "core")
    in_specs = (P(rows, None), P("core", None), P(rows), P(rows))
    out_specs = (P("core", None), P(rows))
    return jax.shard_map(shards, mesh=grid, in_specs=in_specs, out_specs=out_specs, check_vma=False)
```

```python
import jax
import jax.numpy as jnp
from jax import lax
from jax.experimental import pallas as pl
from jax.experimental.pallas import tpu as pltpu
from jax.sharding import Mesh
from jax.sharding import PartitionSpec as P

F32, BF16, I32 = jnp.float32, jnp.bfloat16, jnp.int32
LEVELS = 32767.0
NT = (((1,), (1,)), ((), ()))
VM = pl.BlockSpec(memory_space=pltpu.VMEM)
SM = pl.BlockSpec(memory_space=pltpu.SMEM)
NEAR = (0, -1, 1, 2)


def iota(shape, dim):
    return lax.broadcasted_iota(I32, shape, dim)


def sums_kernel(pos_ref, x_ref, after_ref, own_ref, send_ref):
    step = pl.program_id(0)

    @pl.when(step == 0)
    def _():
        own_ref[...] = jnp.zeros_like(own_ref)
        send_ref[...] = jnp.zeros_like(send_ref)

    z, core = pos_ref[0], pos_ref[3]
    picks, masks, count_rows, count_cols = [], [], [], []
    for s in range(x_ref.shape[0]):
        rows = x_ref.shape[2]
        digits = x_ref[s, 64:72, :].astype(F32)
        code = (digits[0:1] * 64.0 + digits[1:2]).astype(I32)
        low, high = code & 1023, code >> 10
        fine = (iota((32, rows), 0) == (low & 31)).astype(BF16)
        coarse = low >> 5
        picks.append(
            jnp.concatenate([fine * (coarse == h).astype(BF16) for h in range(32)], axis=0)
        )
        pts = x_ref[s, 0:64, :]
        masks.append(
            jnp.concatenate(
                [pts * (high == (b ^ (2 * core))).astype(BF16) for b in range(4)], axis=0
            )
        )
        slot = jnp.where(code < 4096, (low & 31) * 4 + high, -1)
        count_rows.append((iota((32, rows), 0) == coarse).astype(BF16))
        count_cols.append((iota((128, rows), 0) == slot).astype(BF16))
    pick, masked = jnp.concatenate(picks, 1), jnp.concatenate(masks, 1)
    part = lax.dot_general(pick, masked, NT, preferred_element_type=F32)
    counts = lax.dot_general(
        jnp.concatenate(count_rows, 1),
        jnp.concatenate(count_cols, 1),
        NT,
        preferred_element_type=F32,
    )
    for k in range(8):
        at = (k - z) & 7
        own_ref[at, 0:128, :] += part[k * 128 : k * 128 + 128, 0:128]
        send_ref[at, 0:128, :] += part[k * 128 : k * 128 + 128, 128:256]
        own_ref[at, 128:132, :] += counts[k * 4 : k * 4 + 4]
        send_ref[at, 128:132, :] += counts[k * 4 : k * 4 + 4]


def partial_sums(pos, x, after):
    many = 4
    return pl.pallas_call(
        sums_kernel,
        grid_spec=pltpu.PrefetchScalarGridSpec(
            num_scalar_prefetch=1,
            grid=(x.shape[0] // many,),
            in_specs=[
                pl.BlockSpec((many, 72, 512), lambda s, c: (s, 0, 0)),
                pl.BlockSpec(memory_space=pl.ANY),
            ],
            out_specs=[pl.BlockSpec((8, 136, 128), lambda s, c: (0, 0, 0))] * 2,
        ),
        out_shape=[jax.ShapeDtypeStruct((8, 136, 128), F32)] * 2,
        compiler_params=pltpu.CompilerParams(dimension_semantics=("arbitrary",)),
        name="partial_sums",
    )(pos, x, after)


def add_kernel(own_ref, other_ref, *outs):
    for k, out in enumerate(outs):
        out[...] = own_ref[k] + other_ref[k]


def add_pieces(own, other):
    return pl.pallas_call(
        add_kernel,
        in_specs=[VM] * 2,
        out_specs=[VM] * 8,
        out_shape=[jax.ShapeDtypeStruct((136, 128), F32)] * 8,
        name="add_pieces",
    )(own, other)


def mean_kernel(pos_ref, prior_ref, *refs):
    parts, w_ref = refs[:8], refs[8]
    total = parts[0][...]
    for part in parts[1:]:
        total = total + part[...]
    sums, counts = total[0:128], total[128:132]
    core = pos_ref[3]
    row, lane = iota((128, 128), 0), iota((128, 128), 1)
    wide = jnp.concatenate([jnp.broadcast_to(counts[k : k + 1], (32, 128)) for k in range(4)], 0)
    wide = jnp.where((lane >> 2) == (row & 31), wide, 0.0)
    spread = ((row & 3) == (lane >> 6) + 2 * core).astype(F32)
    count = jnp.dot(wide, spread, precision=lax.Precision.HIGHEST, preferred_element_type=F32)
    mean = jnp.where(count > 0.5, sums / jnp.maximum(count, 1.0), prior_ref[...].astype(F32))
    peak = jnp.max(jnp.abs(mean), axis=0, keepdims=True)
    power = jnp.ceil(jnp.log2(jnp.maximum(peak, 1e-30)))
    q = jnp.round(mean * (LEVELS * jnp.exp2(-power)))
    q = jnp.clip(q, -LEVELS, LEVELS).astype(I32)
    w_ref[0:64, :] = (q[0:64] & 0xFFFF) | (q[64:128] << 16)
    w_ref[64:72, :] = jnp.broadcast_to(power.astype(I32), (8, 128))


def encoded_mean(pos, prior, parts):
    return pl.pallas_call(
        mean_kernel,
        in_specs=[SM] + [VM] * 9,
        out_specs=VM,
        out_shape=jax.ShapeDtypeStruct((72, 128), I32),
        name="encoded_mean",
    )(pos, prior, *parts)


def pack_kernel(*refs):
    for c in range(4):
        out = refs[8 + c]
        for h in range(2):
            out[h * 64 : h * 64 + 64, :] = refs[2 * c + h][0:64, :]
        out[128:136, :] = jnp.where(
            iota((8, 128), 0) == 0, refs[2 * c][64:72, :], refs[2 * c + 1][64:72, :]
        )


def pack(blocks):
    return pl.pallas_call(
        pack_kernel,
        in_specs=[VM] * 8,
        out_specs=[VM] * 4,
        out_shape=[jax.ShapeDtypeStruct((136, 128), I32)] * 4,
        name="pack",
    )(*blocks)


def spread_kernel(pos_ref, *refs):
    ins, out_ref = refs[:16], refs[16]
    step = pl.program_id(0)
    y, x = pos_ref[1], pos_ref[2]
    odd_x = (x & 1) == 1
    left = iota((64, 128), 1) < 64

    def halves(word, power):
        scale = jnp.exp2(power.astype(F32)) * (1.0 / LEVELS)
        return ((word << 16) >> 16).astype(F32) * scale, (word >> 16).astype(F32) * scale

    def tile(even, odd, lanes):
        for b, merge in enumerate(
            (
                lambda e, o, m: jnp.where(m, e, pltpu.roll(o, 64, 1)),
                lambda e, o, m: jnp.where(m, pltpu.roll(e, 64, 1), o),
            )
        ):
            word = merge(even[0], odd[0], left)
            power = merge(even[1], odd[1], left[0:8])[0:1]
            first, second = halves(word, power)
            out_ref[b, 0, 0:64, lanes] = first
            out_ref[b, 0, 64:128, lanes] = second

    def fill(block_of, h):
        for j, dy in enumerate(NEAR):
            got = []
            for i in range(4):
                ref, at = block_of(i, j)
                scales = jnp.broadcast_to(ref[at, pl.ds(128 + h, 1), :], (8, 128))
                got.append((ref[at, pl.ds(pl.multiple_of(h * 64, 64), 64), :], scales))

            def choose(p, q):
                return tuple(jnp.where(odd_x, s, t) for s, t in zip(got[p], got[q]))

            at_y = ((y + dy) & 3) * 2
            near = at_y + (x >> 1)
            far = at_y + 1 - (x >> 1)
            tile(choose(1, 0), choose(0, 2), pl.ds(pl.multiple_of(near * 128, 128), 128))
            tile(choose(2, 3), choose(3, 1), pl.ds(pl.multiple_of(far * 128, 128), 128))

    for c in range(4):
        mine = ins[4 * c : 4 * c + 4]

        @pl.when((step >> 1) == c)
        def _():
            if c < 2:
                fill(lambda i, j: (mine[i], j), step & 1)
            else:
                fill(lambda i, j: (mine[j], i), step & 1)


def spread(pos, arrays):
    return pl.pallas_call(
        spread_kernel,
        grid_spec=pltpu.PrefetchScalarGridSpec(
            num_scalar_prefetch=1,
            grid=(8,),
            in_specs=[pl.BlockSpec((4, 136, 128), lambda k, p: (0, 0, 0))] * 16,
            out_specs=pl.BlockSpec((2, 1, 128, 1024), lambda k, p: (0, (p[0] - k) & 7, 0, 0)),
        ),
        out_shape=jax.ShapeDtypeStruct((2, 8, 128, 1024), F32),
        compiler_params=pltpu.CompilerParams(dimension_semantics=("arbitrary",)),
        name="spread",
    )(pos, *arrays)


def shift(v, axis, by):
    size = lax.axis_size(axis)
    return lax.ppermute(v, axis, [(i, (i + by) % size) for i in range(size)])


def rings(first, second, axis):
    behind0, ahead1 = shift(first, axis, 1), shift(second, axis, -1)
    behind1, ahead0 = shift(second, axis, 1), shift(first, axis, -1)
    far0, far1 = shift(behind0, axis, 1), shift(ahead1, axis, -1)
    return (first, behind0, ahead0, far0), (second, behind1, ahead1, far1)


def shards(points, centroids, assign, keep_mask):
    width = points.shape[1]
    swap = [(0, 1), (1, 0)]
    pos = jnp.stack([lax.axis_index(n) for n in ("z", "y", "x", "core")]).astype(I32)
    other = lax.ppermute(centroids, "core", swap)

    code = jnp.where(keep_mask == 1, assign, 4096)
    digits = jnp.stack([code >> 6, code & 63]).astype(BF16)
    digits = jnp.concatenate([digits, jnp.zeros((6, 512), BF16)], axis=0)
    columns = points.T.reshape(16, 64, 512)
    x = jnp.concatenate([columns, jnp.broadcast_to(digits[None], (16, 8, 512))], axis=1)
    x = lax.all_to_all(x, ("y", "x"), 0, 0)

    point_f = points.astype(F32)
    point_sq = jnp.sum(point_f * point_f, axis=1)

    def nearest(c):
        inner = lax.dot_general(points, c, NT, preferred_element_type=F32)
        c_f = c.astype(F32)
        return jnp.min(jnp.sum(c_f * c_f, axis=1)[None, :] - 2.0 * inner, axis=1)

    row_cost = (point_sq + jnp.minimum(nearest(centroids), nearest(other))) / width
    plane = pos[1] * 4 + pos[2]
    prior = lax.dynamic_slice(
        centroids.reshape(2, 8, 128, width), (0, pos[0], 0, plane * 64), (2, 1, 128, 64)
    )
    prior = prior.reshape(2, 128, 64).transpose(1, 0, 2).reshape(128, 128)

    own, send = partial_sums(pos, x, row_cost)
    pieces = add_pieces(own, lax.ppermute(send, "core", swap))
    parts = [pieces[0]] + [shift(pieces[k], "z", k) for k in range(1, 8)]
    w = encoded_mean(pos, prior, parts)
    blocks = [w] + [shift(w, "z", k) for k in range(1, 8)]
    a0, a1, b0, b1 = pack(blocks)
    a0, a1 = (jnp.stack(v) for v in rings(a0, a1, "y"))
    b0, b1 = (jnp.stack(v) for v in rings(b0, b1, "x"))
    a0, a1 = rings(a0, a1, "x")
    b0, b1 = rings(b0, b1, "y")
    new_centroids = spread(pos, (*a0, *a1, *b0, *b1)).reshape(2048, width)
    return new_centroids, row_cost


def solution(mesh):
    grid = Mesh(mesh.devices.reshape(8, 4, 4, 2), ("z", "y", "x", "core"))
    rows = ("z", "y", "x", "core")
    in_specs = (P(rows, None), P("core", None), P(rows), P(rows))
    out_specs = (P("core", None), P(rows))
    return jax.shard_map(shards, mesh=grid, in_specs=in_specs, out_specs=out_specs, check_vma=False)
```

```python
import jax
import jax.numpy as jnp
from jax import lax
from jax.experimental import pallas as pl
from jax.experimental.pallas import tpu as pltpu
from jax.sharding import Mesh
from jax.sharding import PartitionSpec as P

F32, BF16, I32 = jnp.float32, jnp.bfloat16, jnp.int32
LEVELS = 32767.0
NT = (((1,), (1,)), ((), ()))
VM = pl.BlockSpec(memory_space=pltpu.VMEM)
SM = pl.BlockSpec(memory_space=pltpu.SMEM)
PARAMS = pltpu.CompilerParams(vmem_limit_bytes=24 << 20)


def near(*arrays):
    return [pltpu.with_memory_space_constraint(a, pltpu.VMEM) for a in arrays]


def vmem(shape, dtype):
    return pltpu.VMEM(shape, dtype)


def iota(shape, dim):
    return lax.broadcasted_iota(I32, shape, dim)


def sums_kernel(pos_ref, x_ref, after_ref, own_ref, send_ref):
    step = pl.program_id(0)

    @pl.when(step == 0)
    def _():
        own_ref[...] = jnp.zeros_like(own_ref)
        send_ref[...] = jnp.zeros_like(send_ref)

    z, core = pos_ref[0], pos_ref[3]
    picks, masks, count_rows, count_cols = [], [], [], []
    for s in range(4):
        rows = x_ref.shape[2]
        at = step * 4 + s
        digits = x_ref[at, 64:72, :].astype(F32)
        code = (digits[0:1] * 64.0 + digits[1:2]).astype(I32)
        low, high = code & 1023, code >> 10
        fine = (iota((32, rows), 0) == (low & 31)).astype(BF16)
        coarse = low >> 5
        picks.append(
            jnp.concatenate([fine * (coarse == h).astype(BF16) for h in range(32)], axis=0)
        )
        pts = x_ref[at, 0:64, :]
        masks.append(
            jnp.concatenate(
                [pts * (high == (b ^ (2 * core))).astype(BF16) for b in range(4)], axis=0
            )
        )
        slot = jnp.where(code < 4096, (low & 31) * 4 + high, -1)
        count_rows.append((iota((32, rows), 0) == coarse).astype(BF16))
        count_cols.append((iota((128, rows), 0) == slot).astype(BF16))
    pick, masked = jnp.concatenate(picks, 1), jnp.concatenate(masks, 1)
    part = lax.dot_general(pick, masked, NT, preferred_element_type=F32)
    counts = lax.dot_general(
        jnp.concatenate(count_rows, 1),
        jnp.concatenate(count_cols, 1),
        NT,
        preferred_element_type=F32,
    )
    for k in range(8):
        at = (k - z) & 7
        own_ref[at, 0:128, :] += part[k * 128 : k * 128 + 128, 0:128]
        send_ref[at, 0:128, :] += part[k * 128 : k * 128 + 128, 128:256]
        own_ref[at, 128:132, :] += counts[k * 4 : k * 4 + 4]
        send_ref[at, 128:132, :] += counts[k * 4 : k * 4 + 4]


def partial_sums(pos, x, after):
    return pl.pallas_call(
        sums_kernel,
        grid_spec=pltpu.PrefetchScalarGridSpec(
            num_scalar_prefetch=1,
            grid=(x.shape[0] // 4,),
            in_specs=[VM, pl.BlockSpec(memory_space=pl.ANY)],
            out_specs=[VM] * 2,
        ),
        out_shape=[vmem((8, 136, 128), F32)] * 2,
        compiler_params=PARAMS,
        name="partial_sums",
    )(pos, *near(x), after)


def add_kernel(own_ref, other_ref, *outs):
    for k, out in enumerate(outs):
        out[...] = own_ref[k] + other_ref[k]


def add_pieces(own, other):
    return pl.pallas_call(
        add_kernel,
        in_specs=[VM] * 2,
        out_specs=[VM] * 8,
        out_shape=[vmem((136, 128), F32)] * 8,
        compiler_params=PARAMS,
        name="add_pieces",
    )(*near(own, other))


def mean_kernel(pos_ref, prior_ref, *refs):
    parts, w_ref = refs[:8], refs[8]
    total = parts[0][...]
    for part in parts[1:]:
        total = total + part[...]
    sums, counts = total[0:128], total[128:132]
    core = pos_ref[3]
    row, lane = iota((128, 128), 0), iota((128, 128), 1)
    wide = jnp.concatenate([jnp.broadcast_to(counts[k : k + 1], (32, 128)) for k in range(4)], 0)
    wide = jnp.where((lane >> 2) == (row & 31), wide, 0.0)
    spread = ((row & 3) == (lane >> 6) + 2 * core).astype(F32)
    count = jnp.dot(wide, spread, precision=lax.Precision.HIGHEST, preferred_element_type=F32)
    mean = jnp.where(count > 0.5, sums / jnp.maximum(count, 1.0), prior_ref[...].astype(F32))
    peak = jnp.max(jnp.abs(mean), axis=0, keepdims=True)
    power = jnp.ceil(jnp.log2(jnp.maximum(peak, 1e-30)))
    q = jnp.round(mean * (LEVELS * jnp.exp2(-power)))
    q = jnp.clip(q, -LEVELS, LEVELS).astype(I32)
    w_ref[0:64, :] = (q[0:64] & 0xFFFF) | (q[64:128] << 16)
    w_ref[64:72, :] = jnp.broadcast_to(power.astype(I32), (8, 128))


def encoded_mean(pos, prior, parts):
    return pl.pallas_call(
        mean_kernel,
        in_specs=[SM] + [VM] * 9,
        out_specs=VM,
        out_shape=vmem((72, 128), I32),
        compiler_params=PARAMS,
        name="encoded_mean",
    )(pos, *near(prior, *parts))


def pack_kernel(*refs):
    for c in range(2):
        out = refs[8 + c]
        for k in range(4):
            out[k // 2, (k % 2) * 64 : (k % 2) * 64 + 64, :] = refs[4 * c + k][0:64, :]
        for h in range(2):
            out[h, 128:136, :] = jnp.where(
                iota((8, 128), 0) == 0,
                refs[4 * c + 2 * h][64:72, :],
                refs[4 * c + 2 * h + 1][64:72, :],
            )


def pack(blocks):
    return pl.pallas_call(
        pack_kernel,
        in_specs=[VM] * 8,
        out_specs=[VM] * 2,
        out_shape=[vmem((2, 136, 128), I32)] * 2,
        compiler_params=PARAMS,
        name="pack",
    )(*near(*blocks))


def spread_kernel(pos_ref, *refs):
    ins, out_ref = refs[:16], refs[16]
    step = pl.program_id(0)
    y, x = pos_ref[1], pos_ref[2]
    odd_x = (x & 1) == 1
    left = iota((64, 128), 1) < 64

    def halves(word, power):
        scale = jnp.exp2(power.astype(F32)) * (1.0 / LEVELS)
        return ((word << 16) >> 16).astype(F32) * scale, (word >> 16).astype(F32) * scale

    def tile(even, odd, lanes):
        for b, merge in enumerate(
            (
                lambda e, o, m: jnp.where(m, e, pltpu.roll(o, 64, 1)),
                lambda e, o, m: jnp.where(m, pltpu.roll(e, 64, 1), o),
            )
        ):
            word = merge(even[0], odd[0], left)
            power = merge(even[1], odd[1], left[0:8])[0:1]
            first, second = halves(word, power)
            out_ref[b, 0, 0:64, lanes] = first
            out_ref[b, 0, 64:128, lanes] = second

    def fill(block_of, h):
        for dy in range(4):
            got = []
            for dx in range(4):
                ref, at = block_of(dx, dy)
                scales = jnp.broadcast_to(ref[at, pl.ds(128 + h, 1), :], (8, 128))
                got.append((ref[at, pl.ds(pl.multiple_of(h * 64, 64), 64), :], scales))

            def choose(p, q):
                return tuple(jnp.where(odd_x, s, t) for s, t in zip(got[p], got[q]))

            at_y = ((y + dy) & 3) * 2
            own = at_y + (x >> 1)
            far = at_y + 1 - (x >> 1)
            tile(choose(3, 0), choose(0, 1), pl.ds(pl.multiple_of(own * 128, 128), 128))
            tile(choose(1, 2), choose(2, 3), pl.ds(pl.multiple_of(far * 128, 128), 128))

    for c in range(4):
        mine = ins[4 * c : 4 * c + 4]

        @pl.when((step >> 1) == c)
        def _():
            if c < 2:
                fill(lambda dx, dy: (mine[dx], dy), step & 1)
            else:
                fill(lambda dx, dy: (mine[dy], dx), step & 1)


def spread(pos, arrays):
    return pl.pallas_call(
        spread_kernel,
        grid_spec=pltpu.PrefetchScalarGridSpec(
            num_scalar_prefetch=1,
            grid=(8,),
            in_specs=[VM] * 16,
            out_specs=pl.BlockSpec((2, 1, 128, 1024), lambda k, p: (0, (p[0] - k) & 7, 0, 0)),
        ),
        out_shape=jax.ShapeDtypeStruct((2, 8, 128, 1024), F32),
        compiler_params=PARAMS,
        name="spread",
    )(pos, *near(*arrays))


def shift(v, axis, by):
    size = lax.axis_size(axis)
    return lax.ppermute(v, axis, [(i, (i + by) % size) for i in range(size)])


def ring(v, axis):
    behind, ahead = shift(v, axis, 1), shift(v, axis, -1)
    return jnp.stack([v, ahead, shift(behind, axis, 1), behind])


def rings(first, second, axis):
    behind0, ahead1 = shift(first, axis, 1), shift(second, axis, -1)
    behind1, ahead0 = shift(second, axis, 1), shift(first, axis, -1)
    far0, far1 = shift(behind0, axis, 1), shift(ahead1, axis, -1)
    return (first, ahead0, far0, behind0), (second, ahead1, far1, behind1)


def shards(points, centroids, assign, keep_mask):
    width = points.shape[1]
    swap = [(0, 1), (1, 0)]
    pos = jnp.stack([lax.axis_index(n) for n in ("z", "y", "x", "core")]).astype(I32)
    other = lax.ppermute(centroids, "core", swap)

    code = jnp.where(keep_mask == 1, assign, 4096)
    digits = jnp.stack([code >> 6, code & 63]).astype(BF16)
    digits = jnp.concatenate([digits, jnp.zeros((6, 512), BF16)], axis=0)
    columns = points.T.reshape(16, 64, 512)
    x = jnp.concatenate([columns, jnp.broadcast_to(digits[None], (16, 8, 512))], axis=1)
    x = lax.all_to_all(x, ("y", "x"), 0, 0)

    point_f = points.astype(F32)
    point_sq = jnp.sum(point_f * point_f, axis=1)

    def nearest(c):
        inner = lax.dot_general(points, c, NT, preferred_element_type=F32)
        c_f = c.astype(F32)
        return jnp.min(jnp.sum(c_f * c_f, axis=1)[None, :] - 2.0 * inner, axis=1)

    row_cost = (point_sq + jnp.minimum(nearest(centroids), nearest(other))) / width
    plane = pos[1] * 4 + pos[2]
    prior = lax.dynamic_slice(
        centroids.reshape(2, 8, 128, width), (0, pos[0], 0, plane * 64), (2, 1, 128, 64)
    )
    prior = prior.reshape(2, 128, 64).transpose(1, 0, 2).reshape(128, 128)

    own, send = partial_sums(pos, x, row_cost)
    pieces = add_pieces(own, lax.ppermute(send, "core", swap))
    parts = [pieces[0]] + [shift(pieces[k], "z", k) for k in range(1, 8)]
    w = encoded_mean(pos, prior, parts)
    blocks = [w] + [shift(w, "z", k) for k in range(1, 8)]
    a, b = pack(blocks)
    a, b = ring(a, "y"), ring(b, "x")
    a0, a1 = rings(a[:, 0], a[:, 1], "x")
    b0, b1 = rings(b[:, 0], b[:, 1], "y")
    new_centroids = spread(pos, (*a0, *a1, *b0, *b1)).reshape(2048, width)
    return new_centroids, row_cost


def solution(mesh):
    grid = Mesh(mesh.devices.reshape(8, 4, 4, 2), ("z", "y", "x", "core"))
    rows = ("z", "y", "x", "core")
    in_specs = (P(rows, None), P("core", None), P(rows), P(rows))
    out_specs = (P("core", None), P(rows))
    return jax.shard_map(shards, mesh=grid, in_specs=in_specs, out_specs=out_specs, check_vma=False)
```

```python
import jax
import jax.numpy as jnp
from jax import lax
from jax.experimental import pallas as pl
from jax.experimental.pallas import tpu as pltpu
from jax.sharding import Mesh
from jax.sharding import PartitionSpec as P

F32, BF16, I32 = jnp.float32, jnp.bfloat16, jnp.int32
LEVELS = 32767.0
NT = (((1,), (1,)), ((), ()))
VM = pl.BlockSpec(memory_space=pltpu.VMEM)
SM = pl.BlockSpec(memory_space=pltpu.SMEM)
PARAMS = pltpu.CompilerParams(vmem_limit_bytes=24 << 20)


def near(*arrays):
    return [pltpu.with_memory_space_constraint(a, pltpu.VMEM) for a in arrays]


def far(*arrays):
    return [pltpu.with_memory_space_constraint(a, pltpu.HBM) for a in arrays]


def vmem(shape, dtype):
    return pltpu.VMEM(shape, dtype)


def iota(shape, dim):
    return lax.broadcasted_iota(I32, shape, dim)


def rows_kernel(points_ref, assign_ref, keep_ref, out_ref):
    step = pl.program_id(0)
    turned = points_ref[...].T
    for s in range(32):
        out_ref[s, pl.ds(pl.multiple_of(step * 32, 32), 32), :] = turned[s * 32 : s * 32 + 32]

    @pl.when(step == 0)
    def _():
        code = jnp.where(keep_ref[...] == 1, assign_ref[...], 4096)
        digits = jnp.concatenate([code >> 6, code & 63], axis=0).astype(F32).astype(BF16)
        for s in range(32):
            out_ref[s, 128:136, :] = digits


def rows_by_columns(points, assign, keep_mask):
    flat = pl.BlockSpec((4, 128), lambda c: (0, 0))
    return pl.pallas_call(
        rows_kernel,
        grid=(4,),
        in_specs=[pl.BlockSpec((128, 1024), lambda c: (c, 0)), flat, flat],
        out_specs=VM,
        out_shape=vmem((32, 136, 128), BF16),
        compiler_params=PARAMS,
        name="rows_by_columns",
    )(*far(points, assign.reshape(4, 128), keep_mask.reshape(4, 128)))


def sums_kernel(pos_ref, x_ref, after_ref, own_ref, send_ref):
    step = pl.program_id(0)

    @pl.when(step == 0)
    def _():
        own_ref[...] = jnp.zeros_like(own_ref)
        send_ref[...] = jnp.zeros_like(send_ref)

    zh, core = pos_ref[0], pos_ref[4]
    picks, masks, count_rows, count_cols = [], [], [], []
    for s in range(4):
        block = x_ref[step * 4 + s]
        digits = block[128:136].astype(F32)
        code = digits[0:4] * 64.0 + digits[4:8]
        code = jnp.concatenate([code[c : c + 1] for c in range(4)], axis=1).astype(I32)
        low, high = code & 511, code >> 9
        fine = (iota((32, 512), 0) == (low & 31)).astype(BF16)
        coarse = low >> 5
        picks.append(
            jnp.concatenate([fine * (coarse == h).astype(BF16) for h in range(16)], axis=0)
        )
        pts = jnp.concatenate([block[c * 32 : c * 32 + 32] for c in range(4)], axis=1)
        masks.append(
            jnp.concatenate(
                [pts * (high == (b ^ (4 * core))).astype(BF16) for b in range(8)], axis=0
            )
        )
        slot = jnp.where(code < 4096, (low & 15) * 8 + high, -1)
        count_rows.append((iota((32, 512), 0) == (low >> 4)).astype(BF16))
        count_cols.append((iota((128, 512), 0) == slot).astype(BF16))
    part = lax.dot_general(
        jnp.concatenate(picks, 1), jnp.concatenate(masks, 1), NT, preferred_element_type=F32
    )
    counts = lax.dot_general(
        jnp.concatenate(count_rows, 1),
        jnp.concatenate(count_cols, 1),
        NT,
        preferred_element_type=F32,
    )
    for k in range(4):
        at = (k - zh) & 3
        own_ref[at, 0:128, :] += part[k * 128 : k * 128 + 128, 0:128]
        send_ref[at, 0:128, :] += part[k * 128 : k * 128 + 128, 128:256]
        own_ref[at, 128:136, :] += counts[k * 8 : k * 8 + 8]
        send_ref[at, 128:136, :] += counts[k * 8 : k * 8 + 8]


def partial_sums(pos, x, after):
    return pl.pallas_call(
        sums_kernel,
        grid_spec=pltpu.PrefetchScalarGridSpec(
            num_scalar_prefetch=1,
            grid=(8,),
            in_specs=[VM, pl.BlockSpec(memory_space=pl.ANY)],
            out_specs=[VM] * 2,
        ),
        out_shape=[vmem((4, 136, 128), F32)] * 2,
        compiler_params=PARAMS,
        name="partial_sums",
    )(pos, *near(x), after)


def add_kernel(own_ref, other_ref, *outs):
    for k, out in enumerate(outs):
        out[...] = own_ref[k] + other_ref[k]


def add_pieces(own, other):
    return pl.pallas_call(
        add_kernel,
        in_specs=[VM] * 2,
        out_specs=[VM] * 4,
        out_shape=[vmem((136, 128), F32)] * 4,
        compiler_params=PARAMS,
        name="add_pieces",
    )(*near(own, other))


def mean_kernel(pos_ref, prior_ref, *refs):
    parts, w_ref = refs[:4], refs[4]
    total = (parts[0][...] + parts[1][...]) + (parts[2][...] + parts[3][...])
    sums, counts = total[0:128], total[128:136]
    core = pos_ref[4]
    row, lane = iota((128, 128), 0), iota((128, 128), 1)
    wide = jnp.concatenate([jnp.broadcast_to(counts[k : k + 1], (16, 128)) for k in range(8)], 0)
    wide = jnp.where((lane >> 3) == (row & 15), wide, 0.0)
    spread = ((row & 7) == (lane >> 5) + 4 * core).astype(F32)
    count = jnp.dot(wide, spread, precision=lax.Precision.HIGHEST, preferred_element_type=F32)
    mean = jnp.where(count > 0.5, sums / jnp.maximum(count, 1.0), prior_ref[...].astype(F32))
    peak = jnp.max(jnp.abs(mean), axis=0, keepdims=True)
    power = jnp.ceil(jnp.log2(jnp.maximum(peak, 1e-30)))
    q = jnp.round(mean * (LEVELS * jnp.exp2(-power)))
    q = jnp.clip(q, -LEVELS, LEVELS).astype(I32)
    w_ref[0:64, :] = (q[0:64] & 0xFFFF) | (q[64:128] << 16)
    w_ref[64:72, :] = jnp.broadcast_to(power.astype(I32), (8, 128))


def encoded_mean(pos, prior, parts):
    return pl.pallas_call(
        mean_kernel,
        in_specs=[SM] + [VM] * 5,
        out_specs=VM,
        out_shape=vmem((72, 128), I32),
        compiler_params=PARAMS,
        name="encoded_mean",
    )(pos, *near(prior, *parts))


def pack_kernel(*refs):
    for c in range(2):
        out = refs[8 + c]
        for k in range(4):
            out[k // 2, (k % 2) * 64 : (k % 2) * 64 + 64, :] = refs[4 * c + k][0:64, :]
        for h in range(2):
            out[h, 128:136, :] = jnp.where(
                iota((8, 128), 0) == 0,
                refs[4 * c + 2 * h][64:72, :],
                refs[4 * c + 2 * h + 1][64:72, :],
            )


def pack(blocks):
    return pl.pallas_call(
        pack_kernel,
        in_specs=[VM] * 8,
        out_specs=[VM] * 2,
        out_shape=[vmem((2, 136, 128), I32)] * 2,
        compiler_params=PARAMS,
        name="pack",
    )(*near(*blocks))


def spread_kernel(pos_ref, *refs):
    ins, out_ref = refs[:16], refs[16]
    step = pl.program_id(0)
    y, x = pos_ref[2], pos_ref[3]
    group = iota((64, 128), 1) >> 5

    def fill(block_of, h):
        for dy in range(4):
            words, powers = [], []
            for dx in range(4):
                ref, at = block_of(dx, dy)
                by = ((x + dx) & 3) * 32
                word = ref[at, pl.ds(pl.multiple_of(h * 64, 64), 64), :]
                power = jnp.broadcast_to(ref[at, pl.ds(128 + h, 1), :], (8, 128))
                words.append(pltpu.roll(word, by, 1))
                powers.append(pltpu.roll(power, by, 1))
            for b in range(4):
                source = (group - b - x) & 3

                def merge(v, source):
                    v = jnp.where(
                        source < 2,
                        jnp.where(source == 0, v[0], v[1]),
                        jnp.where(source == 2, v[2], v[3]),
                    )
                    return pltpu.roll(v, (128 - 32 * b) % 128, 1) if b else v

                word = merge(words, source)
                scale = jnp.exp2(merge(powers, source[0:8]).astype(F32)) * (1.0 / LEVELS)
                lanes = pl.ds(pl.multiple_of(((y + dy) & 3) * 128, 128), 128)
                out_ref[b, 0, 0:64, lanes] = ((word << 16) >> 16).astype(F32) * scale[0:1]
                out_ref[b, 0, 64:128, lanes] = (word >> 16).astype(F32) * scale[0:1]

    for c in range(4):
        mine = ins[4 * c : 4 * c + 4]

        @pl.when((step >> 1) == c)
        def _():
            if c < 2:
                fill(lambda dx, dy: (mine[dx], dy), step & 1)
            else:
                fill(lambda dx, dy: (mine[dy], dx), step & 1)


def place(step, pos_ref):
    z = (pos_ref[0] * 2 + pos_ref[1] - step) & 7
    return 0, z >> 1, 0, z & 1


def spread(pos, arrays):
    return pl.pallas_call(
        spread_kernel,
        grid_spec=pltpu.PrefetchScalarGridSpec(
            num_scalar_prefetch=1,
            grid=(8,),
            in_specs=[VM] * 16,
            out_specs=pl.BlockSpec((4, 1, 128, 512), place),
        ),
        out_shape=jax.ShapeDtypeStruct((4, 4, 128, 1024), F32),
        compiler_params=PARAMS,
        name="spread",
    )(pos, *near(*arrays))


def shift(v, axis, by):
    size = lax.axis_size(axis)
    return lax.ppermute(v, axis, [(i, (i + by) % size) for i in range(size)])


def ring(v, axis):
    behind, ahead = shift(v, axis, 1), shift(v, axis, -1)
    return jnp.stack([v, ahead, shift(behind, axis, 1), behind])


def rings(first, second, axis):
    behind0, ahead1 = shift(first, axis, 1), shift(second, axis, -1)
    behind1, ahead0 = shift(second, axis, 1), shift(first, axis, -1)
    far0, far1 = shift(behind0, axis, 1), shift(ahead1, axis, -1)
    return (first, ahead0, far0, behind0), (second, ahead1, far1, behind1)


def shards(points, centroids, assign, keep_mask):
    width = points.shape[1]
    swap = [(0, 1), (1, 0)]
    pos = jnp.stack([lax.axis_index(n) for n in ("zh", "zl", "y", "x", "core")]).astype(I32)
    other = lax.ppermute(centroids, "core", swap)

    x = rows_by_columns(points, assign, keep_mask)
    x = lax.all_to_all(x, ("zl", "y", "x"), 0, 0)

    point_f = points.astype(F32)
    point_sq = jnp.sum(point_f * point_f, axis=1)

    def nearest(c):
        inner = lax.dot_general(points, c, NT, preferred_element_type=F32)
        c_f = c.astype(F32)
        return jnp.min(jnp.sum(c_f * c_f, axis=1)[None, :] - 2.0 * inner, axis=1)

    row_cost = (point_sq + jnp.minimum(nearest(centroids), nearest(other))) / width
    slice_at = ((pos[1] * 4 + pos[2]) * 4 + pos[3]) * 32
    prior = lax.dynamic_slice(
        centroids.reshape(4, 4, 128, width), (0, pos[0], 0, slice_at), (4, 1, 128, 32)
    )
    prior = prior.reshape(4, 128, 32).transpose(1, 0, 2).reshape(128, 128)

    own, send = partial_sums(pos, x, row_cost)
    pieces = add_pieces(own, lax.ppermute(send, "core", swap))
    parts = [pieces[0]] + [shift(pieces[k], "zh", k) for k in range(1, 4)]
    w = encoded_mean(pos, prior, parts)
    blocks = [w] + [shift(w, ("zh", "zl"), k) for k in range(1, 8)]
    a, b = pack(blocks)
    a, b = ring(a, "y"), ring(b, "x")
    a0, a1 = rings(a[:, 0], a[:, 1], "x")
    b0, b1 = rings(b[:, 0], b[:, 1], "y")
    new_centroids = spread(pos, (*a0, *a1, *b0, *b1)).reshape(2048, width)
    return new_centroids, row_cost


def solution(mesh):
    grid = Mesh(mesh.devices.reshape(4, 2, 4, 4, 2), ("zh", "zl", "y", "x", "core"))
    rows = ("zh", "zl", "y", "x", "core")
    in_specs = (P(rows, None), P("core", None), P(rows), P(rows))
    out_specs = (P("core", None), P(rows))
    return jax.shard_map(shards, mesh=grid, in_specs=in_specs, out_specs=out_specs, check_vma=False)
```

```python
import jax
import jax.numpy as jnp
from jax import lax
from jax.experimental import pallas as pl
from jax.experimental.pallas import tpu as pltpu
from jax.sharding import Mesh
from jax.sharding import PartitionSpec as P

F32, BF16, I32 = jnp.float32, jnp.bfloat16, jnp.int32
LEVELS = 32767.0
NT = (((1,), (1,)), ((), ()))
VM = pl.BlockSpec(memory_space=pltpu.VMEM)
SM = pl.BlockSpec(memory_space=pltpu.SMEM)
PARAMS = pltpu.CompilerParams(vmem_limit_bytes=24 << 20)


def near(*arrays):
    return [pltpu.with_memory_space_constraint(a, pltpu.VMEM) for a in arrays]


def far(*arrays):
    return [pltpu.with_memory_space_constraint(a, pltpu.HBM) for a in arrays]


def vmem(shape, dtype):
    return pltpu.VMEM(shape, dtype)


def iota(shape, dim):
    return lax.broadcasted_iota(I32, shape, dim)


def rows_kernel(points_ref, assign_ref, keep_ref, out_ref):
    step = pl.program_id(0)
    turned = points_ref[...].T
    for s in range(32):
        at = s if s < 16 else 16 + (s % 4) * 4 + (s - 16) // 4
        out_ref[s, pl.ds(pl.multiple_of(step * 32, 32), 32), :] = turned[at * 32 : at * 32 + 32]

    @pl.when(step == 0)
    def _():
        code = jnp.where(keep_ref[...] == 1, assign_ref[...], 4096)
        digits = jnp.concatenate([code >> 6, code & 63], axis=0).astype(F32).astype(BF16)
        for s in range(32):
            out_ref[s, 128:136, :] = digits


def rows_by_columns(points, assign, keep_mask):
    flat = pl.BlockSpec((4, 128), lambda c: (0, 0))
    return pl.pallas_call(
        rows_kernel,
        grid=(4,),
        in_specs=[pl.BlockSpec((128, 1024), lambda c: (c, 0)), flat, flat],
        out_specs=VM,
        out_shape=vmem((32, 136, 128), BF16),
        compiler_params=PARAMS,
        name="rows_by_columns",
    )(*far(points, assign.reshape(4, 128), keep_mask.reshape(4, 128)))


def sums_kernel(pos_ref, x_ref, after_ref, own_ref, send_ref):
    step = pl.program_id(0)

    @pl.when(step == 0)
    def _():
        own_ref[...] = jnp.zeros_like(own_ref)
        send_ref[...] = jnp.zeros_like(send_ref)

    zh, core = pos_ref[0], pos_ref[4]
    picks, masks, count_rows, count_cols = [], [], [], []
    for s in range(4):
        block = x_ref[step * 4 + s]
        digits = block[128:136].astype(F32)
        code = digits[0:4] * 64.0 + digits[4:8]
        code = jnp.concatenate([code[c : c + 1] for c in range(4)], axis=1).astype(I32)
        low, high = code & 511, code >> 9
        fine = (iota((32, 512), 0) == (low & 31)).astype(BF16)
        coarse = low >> 5
        picks.append(
            jnp.concatenate([fine * (coarse == h).astype(BF16) for h in range(16)], axis=0)
        )
        pts = jnp.concatenate([block[c * 32 : c * 32 + 32] for c in range(4)], axis=1)
        mine = [(high == (b ^ (4 * core))).astype(BF16) for b in range(8)]
        masks.append(jnp.concatenate([pts * m for m in mine], axis=0))
        part16 = (iota((16, 512), 0) == (low & 15)).astype(BF16)
        count_rows.append((iota((32, 512), 0) == (low >> 4)).astype(BF16))
        count_cols.append(jnp.concatenate([part16 * m for m in mine], axis=0))
    part = lax.dot_general(
        jnp.concatenate(picks, 1), jnp.concatenate(masks, 1), NT, preferred_element_type=F32
    )
    counts = lax.dot_general(
        jnp.concatenate(count_rows, 1),
        jnp.concatenate(count_cols, 1),
        NT,
        preferred_element_type=F32,
    )
    others = pltpu.roll(counts, 64, 1)
    for k in range(4):
        at = (k - zh) & 3
        own_ref[at, 0:128, :] += part[k * 128 : k * 128 + 128, 0:128]
        send_ref[at, 0:128, :] += part[k * 128 : k * 128 + 128, 128:256]
        own_ref[at, 128:136, :] += counts[k * 8 : k * 8 + 8]
        send_ref[at, 128:136, :] += others[k * 8 : k * 8 + 8]


def partial_sums(pos, x, after):
    return pl.pallas_call(
        sums_kernel,
        grid_spec=pltpu.PrefetchScalarGridSpec(
            num_scalar_prefetch=1,
            grid=(8,),
            in_specs=[VM, pl.BlockSpec(memory_space=pl.ANY)],
            out_specs=[VM] * 2,
        ),
        out_shape=[vmem((4, 136, 128), F32)] * 2,
        compiler_params=PARAMS,
        name="partial_sums",
    )(pos, *near(x), after)


def add_kernel(own_ref, other_ref, *outs):
    for k, out in enumerate(outs):
        out[...] = own_ref[k] + other_ref[k]


def add_pieces(own, other):
    return pl.pallas_call(
        add_kernel,
        in_specs=[VM] * 2,
        out_specs=[VM] * 4,
        out_shape=[vmem((136, 128), F32)] * 4,
        compiler_params=PARAMS,
        name="add_pieces",
    )(*near(own, other))


def mean_kernel(pos_ref, prior_ref, *refs):
    parts, w_ref = refs[:4], refs[4]
    total = (parts[0][...] + parts[1][...]) + (parts[2][...] + parts[3][...])
    sums, counts = total[0:128], total[128:136]
    row, lane = iota((128, 128), 0), iota((128, 128), 1)
    wide = jnp.concatenate([jnp.broadcast_to(counts[k : k + 1], (16, 128)) for k in range(8)], 0)
    wide = jnp.where((lane & 15) == (row & 15), wide, 0.0)
    spread = ((row >> 4) == (lane >> 5)).astype(F32)
    count = jnp.dot(wide, spread, precision=lax.Precision.HIGHEST, preferred_element_type=F32)
    mean = jnp.where(count > 0.5, sums / jnp.maximum(count, 1.0), prior_ref[...].astype(F32))
    peak = jnp.max(jnp.abs(mean), axis=0, keepdims=True)
    power = jnp.ceil(jnp.log2(jnp.maximum(peak, 1e-30)))
    q = jnp.round(mean * (LEVELS * jnp.exp2(-power)))
    q = jnp.clip(q, -LEVELS, LEVELS).astype(I32)
    by = pos_ref[3 - pos_ref[1]] * 32
    w_ref[0:64, :] = pltpu.roll((q[0:64] & 0xFFFF) | (q[64:128] << 16), by, 1)
    w_ref[64:72, :] = pltpu.roll(jnp.broadcast_to(power.astype(I32), (8, 128)), by, 1)


def encoded_mean(pos, prior, parts):
    return pl.pallas_call(
        mean_kernel,
        in_specs=[SM] + [VM] * 5,
        out_specs=VM,
        out_shape=vmem((72, 128), I32),
        compiler_params=PARAMS,
        name="encoded_mean",
    )(pos, *near(prior, *parts))


def pack_kernel(*refs):
    out = refs[4]
    for i in range(4):
        out[i // 2, (i % 2) * 64 : (i % 2) * 64 + 64, :] = refs[i][0:64, :]
    for c in range(2):
        out[c, 128:136, :] = jnp.where(
            iota((8, 128), 0) == 0, refs[2 * c][64:72, :], refs[2 * c + 1][64:72, :]
        )


def pack(blocks):
    return pl.pallas_call(
        pack_kernel,
        in_specs=[VM] * 4,
        out_specs=VM,
        out_shape=vmem((2, 136, 128), I32),
        compiler_params=PARAMS,
        name="pack",
    )(*near(*blocks))


def spread(pos, pieces, out, name):
    many = len(pieces)
    arrays = [chunk for piece in pieces for chunk in piece[2]]

    def kernel(pos_ref, *refs):
        ins, (out_ref, made, sems) = refs[: 2 * many], refs[-3:]
        group = iota((64, 128), 1) >> 5
        copies = []
        for p, (colour, d, _) in enumerate(pieces):
            half = pos_ref[1] ^ colour
            first = pos_ref[3 - half]
            lanes = (half * 4 + ((pos_ref[2 + half] + d) & 3)) * 128
            sources = [(group - b - first) & 3 for b in range(4)]
            for q in range(4):
                ref, h = ins[2 * p + q // 2], q % 2
                words = [ref[k, h * 64 : h * 64 + 64, :] for k in range(4)]
                powers = [
                    jnp.broadcast_to(ref[k, 128 + h : 129 + h, :], (8, 128)) for k in range(4)
                ]
                at = p * 4 + q
                for b in range(4):

                    def merge(v, source):
                        v = jnp.where(
                            source < 2,
                            jnp.where(source == 0, v[0], v[1]),
                            jnp.where(source == 2, v[2], v[3]),
                        )
                        return pltpu.roll(v, (128 - 32 * b) % 128, 1) if b else v

                    word = merge(words, sources[b])
                    power = merge(powers, sources[b][0:8]).astype(F32)
                    scale = (jnp.exp2(power) * (1.0 / LEVELS))[0:1]
                    made[at, b, 0:64, :] = ((word << 16) >> 16).astype(F32) * scale
                    made[at, b, 64:128, :] = (word >> 16).astype(F32) * scale
                copy = pltpu.make_async_copy(
                    made.at[at],
                    out_ref.at[:, (pos_ref[0] - q) & 3, :, pl.ds(pl.multiple_of(lanes, 128), 128)],
                    sems.at[at],
                )
                copy.start()
                copies.append(copy)
        for copy in copies:
            copy.wait()

    old = [] if out is None else [out]
    anywhere = pl.BlockSpec(memory_space=pl.ANY)
    return pl.pallas_call(
        kernel,
        in_specs=[SM] + [VM] * (2 * many) + [anywhere] * len(old),
        out_specs=anywhere,
        out_shape=jax.ShapeDtypeStruct((4, 4, 128, 1024), F32),
        scratch_shapes=[
            pltpu.VMEM((4 * many, 4, 128, 128), F32),
            pltpu.SemaphoreType.DMA((4 * many,)),
        ],
        input_output_aliases={1 + 2 * many: 0} if old else {},
        compiler_params=PARAMS,
        name=name,
    )(pos, *near(*arrays), *old)


def shift(v, axis, by):
    size = lax.axis_size(axis)
    return lax.ppermute(v, axis, [(i, (i + by) % size) for i in range(size)])


def turn(v, way, by):
    pairs = []
    for zl in range(2):
        for y in range(4):
            for x in range(4):
                to = (y, (x + by) % 4) if zl == way else ((y + by) % 4, x)
                pairs.append((zl * 16 + y * 4 + x, zl * 16 + to[0] * 4 + to[1]))
    return lax.ppermute(v, ("zl", "y", "x"), pairs)


def ring(v, way):
    behind, ahead = turn(v, way, 1), turn(v, way, -1)
    return jnp.stack([v, ahead, turn(behind, way, 1), behind])


def rings(v, way):
    first, second = v[:, 0], v[:, 1]
    behind0, ahead1 = turn(first, way, 1), turn(second, way, -1)
    behind1, ahead0 = turn(second, way, 1), turn(first, way, -1)
    far0, far1 = turn(behind0, way, 1), turn(ahead1, way, -1)
    return (first, second), (ahead0, ahead1), (far0, far1), (behind0, behind1)


def shards(points, centroids, assign, keep_mask):
    width = points.shape[1]
    swap = [(0, 1), (1, 0)]
    pos = jnp.stack([lax.axis_index(n) for n in ("zh", "zl", "y", "x", "core")]).astype(I32)
    other = lax.ppermute(centroids, "core", swap)

    x = rows_by_columns(points, assign, keep_mask)
    x = lax.all_to_all(x, ("zl", "y", "x"), 0, 0)

    point_f = points.astype(F32)
    point_sq = jnp.sum(point_f * point_f, axis=1)

    def nearest(c):
        inner = lax.dot_general(points, c, NT, preferred_element_type=F32)
        c_f = c.astype(F32)
        return jnp.min(jnp.sum(c_f * c_f, axis=1)[None, :] - 2.0 * inner, axis=1)

    row_cost = (point_sq + jnp.minimum(nearest(centroids), nearest(other))) / width
    swapped = jnp.where(pos[1] == 0, pos[2] * 4 + pos[3], 16 + pos[3] * 4 + pos[2])
    slice_at = swapped * 32
    prior = lax.dynamic_slice(
        centroids.reshape(4, 4, 128, width), (0, pos[0], 0, slice_at), (4, 1, 128, 32)
    )
    prior = prior.reshape(4, 128, 32).transpose(1, 0, 2).reshape(128, 128)

    own, send = partial_sums(pos, x, row_cost)
    pieces = add_pieces(own, lax.ppermute(send, "core", swap))
    parts = [pieces[0]] + [shift(pieces[k], "zh", k) for k in range(1, 4)]
    w = encoded_mean(pos, prior, parts)
    mine = pack([w] + [shift(w, "zh", k) for k in range(1, 4)])
    theirs = lax.ppermute(mine, "zl", swap)
    colours = rings(ring(mine, 0), 1), rings(ring(theirs, 1), 0)
    both = range(2)
    out = spread(pos, [(c, 0, colours[c][0]) for c in both], None, "spread_own")
    out = spread(pos, [(c, d, colours[c][d]) for c in both for d in (1, 3)], out, "spread_next")
    out = spread(pos, [(c, 2, colours[c][2]) for c in both], out, "spread_far")
    new_centroids = out.reshape(2048, width)
    return new_centroids, row_cost


def solution(mesh):
    grid = Mesh(mesh.devices.reshape(4, 2, 4, 4, 2), ("zh", "zl", "y", "x", "core"))
    rows = ("zh", "zl", "y", "x", "core")
    in_specs = (P(rows, None), P("core", None), P(rows), P(rows))
    out_specs = (P("core", None), P(rows))
    return jax.shard_map(shards, mesh=grid, in_specs=in_specs, out_specs=out_specs, check_vma=False)
```

```python
import jax
import jax.numpy as jnp
from jax import lax
from jax.experimental import pallas as pl
from jax.experimental.pallas import tpu as pltpu
from jax.sharding import Mesh
from jax.sharding import PartitionSpec as P

F32, BF16, I32 = jnp.float32, jnp.bfloat16, jnp.int32
LEVELS = 32767.0
NT = (((1,), (1,)), ((), ()))
VM = pl.BlockSpec(memory_space=pltpu.VMEM)
SM = pl.BlockSpec(memory_space=pltpu.SMEM)
PARAMS = pltpu.CompilerParams(vmem_limit_bytes=24 << 20)


def near(*arrays):
    return [pltpu.with_memory_space_constraint(a, pltpu.VMEM) for a in arrays]


def far(*arrays):
    return [pltpu.with_memory_space_constraint(a, pltpu.HBM) for a in arrays]


def vmem(shape, dtype):
    return pltpu.VMEM(shape, dtype)


def iota(shape, dim):
    return lax.broadcasted_iota(I32, shape, dim)


def rows_kernel(points_ref, assign_ref, keep_ref, out_ref, pts_ref, ids_ref, sems):
    copies = [
        pltpu.make_async_copy(assign_ref, ids_ref.at[0], sems.at[4]),
        pltpu.make_async_copy(keep_ref, ids_ref.at[1], sems.at[5]),
    ]
    for c in range(4):
        part = points_ref.at[c * 128 : c * 128 + 128]
        copies.append(pltpu.make_async_copy(part, pts_ref.at[c], sems.at[c]))
    for copy in copies:
        copy.start()
    for copy in copies[:2]:
        copy.wait()
    code = jnp.where(ids_ref[1] == 1, ids_ref[0], 4096)
    digits = jnp.concatenate([code >> 6, code & 63], axis=0).astype(F32).astype(BF16)
    for s in range(32):
        out_ref[s, 128:136, :] = digits
    for c in range(4):
        copies[2 + c].wait()
        turned = pts_ref[c].T
        for s in range(32):
            at = s if s < 16 else 16 + (s % 4) * 4 + (s - 16) // 4
            out_ref[s, c * 32 : c * 32 + 32, :] = turned[at * 32 : at * 32 + 32]


def rows_by_columns(points, assign, keep_mask):
    return pl.pallas_call(
        rows_kernel,
        in_specs=[pl.BlockSpec(memory_space=pl.ANY)] * 3,
        out_specs=VM,
        out_shape=vmem((32, 136, 128), BF16),
        scratch_shapes=[
            pltpu.VMEM((4, 128, 1024), BF16),
            pltpu.VMEM((2, 4, 128), I32),
            pltpu.SemaphoreType.DMA((6,)),
        ],
        compiler_params=PARAMS,
        name="rows_by_columns",
    )(*far(points, assign.reshape(4, 128), keep_mask.reshape(4, 128)))


def sums_kernel(pos_ref, x_ref, after_ref, own_ref, send_ref):
    step = pl.program_id(0)

    @pl.when(step == 0)
    def _():
        own_ref[...] = jnp.zeros_like(own_ref)
        send_ref[...] = jnp.zeros_like(send_ref)

    zh, core = pos_ref[0], pos_ref[4]
    picks, masks, count_rows, count_cols, tops = [], [], [], [], []
    ids = iota((256, 512), 0).astype(F32).astype(BF16)
    for s in range(16):
        block = x_ref[step * 16 + s]
        digits = block[128:136].astype(F32)
        code = digits[0:4] * 64.0 + digits[4:8]
        code = jnp.concatenate([code[c : c + 1] for c in range(4)], axis=1).astype(I32)
        low, high = code & 511, code >> 9
        for k in range(2):
            key = jnp.where((low >> 8) == k, low & 255, -1).astype(F32).astype(BF16)
            hits = jnp.where(ids == key, jnp.ones((), BF16), jnp.zeros((), BF16))
            tops.append(hits)
        picks.append(jnp.concatenate(tops[-2:], axis=0))
        pts = jnp.concatenate([block[c * 32 : c * 32 + 32] for c in range(4)], axis=1)
        group = (high ^ (4 * core)).astype(F32).astype(BF16)
        wide = jnp.broadcast_to(group, (32, 512))
        zero = jnp.zeros((), BF16)
        masks.append(jnp.concatenate([jnp.where(wide == b, pts, zero) for b in range(8)], axis=0))
        part16 = (iota((16, 512), 0) == (low & 15)).astype(BF16)
        count_rows.append((iota((32, 512), 0) == (low >> 4)).astype(BF16))
        count_cols.append(
            jnp.concatenate([jnp.where(wide[0:16] == b, part16, zero) for b in range(8)], axis=0)
        )
    part = lax.dot_general(
        jnp.concatenate(picks, 1), jnp.concatenate(masks, 1), NT, preferred_element_type=F32
    )
    counts = lax.dot_general(
        jnp.concatenate(count_rows, 1),
        jnp.concatenate(count_cols, 1),
        NT,
        preferred_element_type=F32,
    )
    others = pltpu.roll(counts, 64, 1)
    for k in range(4):
        at = (k - zh) & 3
        own_ref[at, 0:128, :] += part[k * 128 : k * 128 + 128, 0:128]
        send_ref[at, 0:128, :] += part[k * 128 : k * 128 + 128, 128:256]
        own_ref[at, 128:136, :] += counts[k * 8 : k * 8 + 8]
        send_ref[at, 128:136, :] += others[k * 8 : k * 8 + 8]


def partial_sums(pos, x, after):
    return pl.pallas_call(
        sums_kernel,
        grid_spec=pltpu.PrefetchScalarGridSpec(
            num_scalar_prefetch=1,
            grid=(2,),
            in_specs=[VM, pl.BlockSpec(memory_space=pl.ANY)],
            out_specs=[VM] * 2,
        ),
        out_shape=[vmem((4, 136, 128), F32)] * 2,
        compiler_params=PARAMS,
        name="partial_sums",
    )(pos, *near(x), after)


def add_kernel(own_ref, other_ref, *outs):
    for k, out in enumerate(outs):
        out[...] = own_ref[k] + other_ref[k]


def add_pieces(own, other):
    return pl.pallas_call(
        add_kernel,
        in_specs=[VM] * 2,
        out_specs=[VM] * 4,
        out_shape=[vmem((136, 128), F32)] * 4,
        compiler_params=PARAMS,
        name="add_pieces",
    )(*near(own, other))


def mean_kernel(pos_ref, prior_ref, *refs):
    parts, w_ref = refs[:4], refs[4]
    total = (parts[0][...] + parts[1][...]) + (parts[2][...] + parts[3][...])
    sums, counts = total[0:128], total[128:136]
    row, lane = iota((128, 128), 0), iota((128, 128), 1)
    wide = jnp.concatenate([jnp.broadcast_to(counts[k : k + 1], (16, 128)) for k in range(8)], 0)
    wide = jnp.where((lane & 15) == (row & 15), wide, 0.0)
    spread = ((row >> 4) == (lane >> 5)).astype(F32)
    count = jnp.dot(wide, spread, precision=lax.Precision.HIGHEST, preferred_element_type=F32)
    mean = jnp.where(count > 0.5, sums / jnp.maximum(count, 1.0), prior_ref[...].astype(F32))
    peak = jnp.max(jnp.abs(mean), axis=0, keepdims=True)
    power = jnp.ceil(jnp.log2(jnp.maximum(peak, 1e-30)))
    q = jnp.round(mean * (LEVELS * jnp.exp2(-power)))
    q = jnp.clip(q, -LEVELS, LEVELS).astype(I32)
    by = pos_ref[3 - pos_ref[1]] * 32
    w_ref[0:64, :] = pltpu.roll((q[0:64] & 0xFFFF) | (q[64:128] << 16), by, 1)
    w_ref[64:72, :] = pltpu.roll(jnp.broadcast_to(power.astype(I32), (8, 128)), by, 1)


def encoded_mean(pos, prior, parts):
    return pl.pallas_call(
        mean_kernel,
        in_specs=[SM] + [VM] * 5,
        out_specs=VM,
        out_shape=vmem((72, 128), I32),
        compiler_params=PARAMS,
        name="encoded_mean",
    )(pos, *near(prior, *parts))


def pack_kernel(*refs):
    out = refs[4]
    for i in range(4):
        out[i // 2, (i % 2) * 64 : (i % 2) * 64 + 64, :] = refs[i][0:64, :]
    for c in range(2):
        out[c, 128:136, :] = jnp.where(
            iota((8, 128), 0) == 0, refs[2 * c][64:72, :], refs[2 * c + 1][64:72, :]
        )


def pack(blocks):
    return pl.pallas_call(
        pack_kernel,
        in_specs=[VM] * 4,
        out_specs=VM,
        out_shape=vmem((2, 136, 128), I32),
        compiler_params=PARAMS,
        name="pack",
    )(*near(*blocks))


def spread(pos, pieces, out, name):
    many = len(pieces)
    arrays = [chunk for piece in pieces for chunk in piece[2]]

    def kernel(pos_ref, *refs):
        ins, (out_ref, made, sems) = refs[: 2 * many], refs[-3:]
        group = iota((64, 128), 1) >> 5
        copies = []
        for p, (colour, d, _) in enumerate(pieces):
            half = pos_ref[1] ^ colour
            first = pos_ref[3 - half]
            lanes = (half * 4 + ((pos_ref[2 + half] + d) & 3)) * 128
            sources = [(group - b - first) & 3 for b in range(4)]
            for q in range(4):
                ref, h = ins[2 * p + q // 2], q % 2
                words = [ref[k, h * 64 : h * 64 + 64, :] for k in range(4)]
                powers = [
                    jnp.broadcast_to(ref[k, 128 + h : 129 + h, :], (8, 128)) for k in range(4)
                ]
                at = p * 4 + q
                for b in range(4):

                    def merge(v, source):
                        v = jnp.where(
                            source < 2,
                            jnp.where(source == 0, v[0], v[1]),
                            jnp.where(source == 2, v[2], v[3]),
                        )
                        return pltpu.roll(v, (128 - 32 * b) % 128, 1) if b else v

                    word = merge(words, sources[b])
                    power = merge(powers, sources[b][0:8]).astype(F32)
                    scale = (jnp.exp2(power) * (1.0 / LEVELS))[0:1]
                    made[at, b, 0:64, :] = ((word << 16) >> 16).astype(F32) * scale
                    made[at, b, 64:128, :] = (word >> 16).astype(F32) * scale
                copy = pltpu.make_async_copy(
                    made.at[at],
                    out_ref.at[:, (pos_ref[0] - q) & 3, :, pl.ds(pl.multiple_of(lanes, 128), 128)],
                    sems.at[at],
                )
                copy.start()
                copies.append(copy)
        for copy in copies:
            copy.wait()

    old = [] if out is None else [out]
    anywhere = pl.BlockSpec(memory_space=pl.ANY)
    return pl.pallas_call(
        kernel,
        in_specs=[SM] + [VM] * (2 * many) + [anywhere] * len(old),
        out_specs=anywhere,
        out_shape=jax.ShapeDtypeStruct((4, 4, 128, 1024), F32),
        scratch_shapes=[
            pltpu.VMEM((4 * many, 4, 128, 128), F32),
            pltpu.SemaphoreType.DMA((4 * many,)),
        ],
        input_output_aliases={1 + 2 * many: 0} if old else {},
        compiler_params=PARAMS,
        name=name,
    )(pos, *near(*arrays), *old)


def shift(v, axis, by):
    size = lax.axis_size(axis)
    return lax.ppermute(v, axis, [(i, (i + by) % size) for i in range(size)])


def turn(v, way, by):
    pairs = []
    for zl in range(2):
        for y in range(4):
            for x in range(4):
                to = (y, (x + by) % 4) if zl == way else ((y + by) % 4, x)
                pairs.append((zl * 16 + y * 4 + x, zl * 16 + to[0] * 4 + to[1]))
    return lax.ppermute(v, ("zl", "y", "x"), pairs)


def ring(v, way):
    behind, ahead = turn(v, way, 1), turn(v, way, -1)
    return jnp.stack([v, ahead, turn(behind, way, 1), behind])


def rings(v, way):
    first, second = v[:, 0], v[:, 1]
    behind0, ahead1 = turn(first, way, 1), turn(second, way, -1)
    behind1, ahead0 = turn(second, way, 1), turn(first, way, -1)
    far0, far1 = turn(behind0, way, 1), turn(ahead1, way, -1)
    return (first, second), (ahead0, ahead1), (far0, far1), (behind0, behind1)


def shards(points, centroids, assign, keep_mask):
    width = points.shape[1]
    swap = [(0, 1), (1, 0)]
    pos = jnp.stack([lax.axis_index(n) for n in ("zh", "zl", "y", "x", "core")]).astype(I32)
    other = lax.ppermute(centroids, "core", swap)

    x = rows_by_columns(points, assign, keep_mask)
    x = lax.all_to_all(x, ("zl", "y", "x"), 0, 0)

    point_f = points.astype(F32)
    point_sq = jnp.sum(point_f * point_f, axis=1)

    def nearest(c):
        inner = lax.dot_general(points, c, NT, preferred_element_type=F32)
        c_f = c.astype(F32)
        return jnp.min(jnp.sum(c_f * c_f, axis=1)[None, :] - 2.0 * inner, axis=1)

    row_cost = (point_sq + jnp.minimum(nearest(centroids), nearest(other))) / width
    swapped = jnp.where(pos[1] == 0, pos[2] * 4 + pos[3], 16 + pos[3] * 4 + pos[2])
    slice_at = swapped * 32
    prior = lax.dynamic_slice(
        centroids.reshape(4, 4, 128, width), (0, pos[0], 0, slice_at), (4, 1, 128, 32)
    )
    prior = prior.reshape(4, 128, 32).transpose(1, 0, 2).reshape(128, 128)

    own, send = partial_sums(pos, x, row_cost)
    pieces = add_pieces(own, lax.ppermute(send, "core", swap))
    parts = [pieces[0]] + [shift(pieces[k], "zh", k) for k in range(1, 4)]
    w = encoded_mean(pos, prior, parts)
    opposite = shift(w, "zh", 2)
    mine = pack([w, shift(w, "zh", 1), opposite, shift(w, "zh", 3)])
    theirs = lax.ppermute(mine, "zl", swap)
    colours = rings(ring(mine, 0), 1), rings(ring(theirs, 1), 0)
    both = range(2)
    out = spread(pos, [(c, 0, colours[c][0]) for c in both], None, "spread_own")
    out = spread(pos, [(c, d, colours[c][d]) for c in both for d in (1, 3)], out, "spread_next")
    out = spread(pos, [(c, 2, colours[c][2]) for c in both], out, "spread_far")
    new_centroids = out.reshape(2048, width)
    return new_centroids, row_cost


def solution(mesh):
    grid = Mesh(mesh.devices.reshape(4, 2, 4, 4, 2), ("zh", "zl", "y", "x", "core"))
    rows = ("zh", "zl", "y", "x", "core")
    in_specs = (P(rows, None), P("core", None), P(rows), P(rows))
    out_specs = (P("core", None), P(rows))
    return jax.shard_map(shards, mesh=grid, in_specs=in_specs, out_specs=out_specs, check_vma=False)
```

```python
import jax
import jax.numpy as jnp
from jax import lax
from jax.experimental import pallas as pl
from jax.experimental.pallas import tpu as pltpu
from jax.sharding import Mesh
from jax.sharding import PartitionSpec as P


F32, BF16, I32 = jnp.float32, jnp.bfloat16, jnp.int32
LEVELS = 32767.0
NT = (((1,), (1,)), ((), ()))
VM = pl.BlockSpec(memory_space=pltpu.VMEM)
SM = pl.BlockSpec(memory_space=pltpu.SMEM)
PARAMS = pltpu.CompilerParams(vmem_limit_bytes=24 << 20)


def near(*arrays):
    return [pltpu.with_memory_space_constraint(a, pltpu.VMEM) for a in arrays]


def far(*arrays):
    return [pltpu.with_memory_space_constraint(a, pltpu.HBM) for a in arrays]


def vmem(shape, dtype):
    return pltpu.VMEM(shape, dtype)


def iota(shape, dim):
    return lax.broadcasted_iota(I32, shape, dim)


def rows_kernel(points_ref, assign_ref, keep_ref, out_ref, pts_ref, ids_ref, sems):
    copies = [
        pltpu.make_async_copy(assign_ref, ids_ref.at[0], sems.at[4]),
        pltpu.make_async_copy(keep_ref, ids_ref.at[1], sems.at[5]),
    ]
    for c in range(4):
        part = points_ref.at[c * 128 : c * 128 + 128]
        copies.append(pltpu.make_async_copy(part, pts_ref.at[c], sems.at[c]))
    for copy in copies:
        copy.start()
    for copy in copies[:2]:
        copy.wait()
    code = jnp.where(ids_ref[1] == 1, ids_ref[0], 4096)
    digits = jnp.concatenate([code >> 6, code & 63], axis=0).astype(F32).astype(BF16)
    for s in range(32):
        out_ref[s, 128:136, :] = digits
    for c in range(4):
        copies[2 + c].wait()
        turned = pts_ref[c].T
        for s in range(32):
            at = s if s < 16 else 16 + (s % 4) * 4 + (s - 16) // 4
            out_ref[s, c * 32 : c * 32 + 32, :] = turned[at * 32 : at * 32 + 32]


def rows_by_columns(points, assign, keep_mask):
    return pl.pallas_call(
        rows_kernel,
        in_specs=[pl.BlockSpec(memory_space=pl.ANY)] * 3,
        out_specs=VM,
        out_shape=vmem((32, 136, 128), BF16),
        scratch_shapes=[
            pltpu.VMEM((4, 128, 1024), BF16),
            pltpu.VMEM((2, 4, 128), I32),
            pltpu.SemaphoreType.DMA((6,)),
        ],
        compiler_params=PARAMS,
        name="rows_by_columns",
    )(*far(points, assign.reshape(4, 128), keep_mask.reshape(4, 128)))


def sums_kernel(pos_ref, x_ref, after_ref, own_ref, send_ref):
    step = pl.program_id(0)

    @pl.when(step == 0)
    def _():
        own_ref[...] = jnp.zeros_like(own_ref)
        send_ref[...] = jnp.zeros_like(send_ref)

    zh, core = pos_ref[0], pos_ref[4]
    picks, masks, count_rows, count_cols, tops = [], [], [], [], []
    ids = iota((256, 512), 0).astype(F32).astype(BF16)
    for s in range(16):
        block = x_ref[step * 16 + s]
        digits = block[128:136].astype(F32)
        code = digits[0:4] * 64.0 + digits[4:8]
        code = jnp.concatenate([code[c : c + 1] for c in range(4)], axis=1).astype(I32)
        low, high = code & 511, code >> 9
        for k in range(2):
            key = jnp.where((low >> 8) == k, low & 255, -1).astype(F32).astype(BF16)
            hits = jnp.where(ids == key, jnp.ones((), BF16), jnp.zeros((), BF16))
            tops.append(hits)
        picks.append(jnp.concatenate(tops[-2:], axis=0))
        pts = jnp.concatenate([block[c * 32 : c * 32 + 32] for c in range(4)], axis=1)
        group = (high ^ (4 * core)).astype(F32).astype(BF16)
        wide = jnp.broadcast_to(group, (32, 512))
        zero = jnp.zeros((), BF16)
        masks.append(jnp.concatenate([jnp.where(wide == b, pts, zero) for b in range(8)], axis=0))
        part16 = (iota((16, 512), 0) == (low & 15)).astype(BF16)
        count_rows.append((iota((32, 512), 0) == (low >> 4)).astype(BF16))
        count_cols.append(
            jnp.concatenate([jnp.where(wide[0:16] == b, part16, zero) for b in range(8)], axis=0)
        )
    part = lax.dot_general(
        jnp.concatenate(picks, 1), jnp.concatenate(masks, 1), NT, preferred_element_type=F32
    )
    counts = lax.dot_general(
        jnp.concatenate(count_rows, 1),
        jnp.concatenate(count_cols, 1),
        NT,
        preferred_element_type=F32,
    )
    others = pltpu.roll(counts, 64, 1)
    for k in range(4):
        at = (k - zh) & 3
        own_ref[at, 0:128, :] += part[k * 128 : k * 128 + 128, 0:128]
        send_ref[at, 0:128, :] += part[k * 128 : k * 128 + 128, 128:256]
        own_ref[at, 128:136, :] += counts[k * 8 : k * 8 + 8]
        send_ref[at, 128:136, :] += others[k * 8 : k * 8 + 8]


def partial_sums(pos, x, after):
    return pl.pallas_call(
        sums_kernel,
        grid_spec=pltpu.PrefetchScalarGridSpec(
            num_scalar_prefetch=1,
            grid=(2,),
            in_specs=[VM, pl.BlockSpec(memory_space=pl.ANY)],
            out_specs=[VM] * 2,
        ),
        out_shape=[vmem((4, 136, 128), F32)] * 2,
        compiler_params=PARAMS,
        name="partial_sums",
    )(pos, *near(x), after)


def add_kernel(own_ref, other_ref, *outs):
    for k, out in enumerate(outs):
        out[...] = own_ref[k] + other_ref[k]


def add_pieces(own, other):
    return pl.pallas_call(
        add_kernel,
        in_specs=[VM] * 2,
        out_specs=[VM] * 4,
        out_shape=[vmem((136, 128), F32)] * 4,
        compiler_params=PARAMS,
        name="add_pieces",
    )(*near(own, other))


def mean_kernel(pos_ref, prior_ref, *refs):
    parts, w_ref = refs[:4], refs[4]
    total = (parts[0][...] + parts[1][...]) + (parts[2][...] + parts[3][...])
    sums, counts = total[0:128], total[128:136]
    row, lane = iota((128, 128), 0), iota((128, 128), 1)
    wide = jnp.concatenate([jnp.broadcast_to(counts[k : k + 1], (16, 128)) for k in range(8)], 0)
    wide = jnp.where((lane & 15) == (row & 15), wide, 0.0)
    spread = ((row >> 4) == (lane >> 5)).astype(F32)
    count = jnp.dot(wide, spread, precision=lax.Precision.HIGHEST, preferred_element_type=F32)
    mean = jnp.where(count > 0.5, sums / jnp.maximum(count, 1.0), prior_ref[...].astype(F32))
    peak = jnp.max(jnp.abs(mean), axis=0, keepdims=True)
    power = jnp.ceil(jnp.log2(jnp.maximum(peak, 1e-30)))
    q = jnp.round(mean * (LEVELS * jnp.exp2(-power)))
    q = jnp.clip(q, -LEVELS, LEVELS).astype(I32)
    by = pos_ref[3 - pos_ref[1]] * 32
    w_ref[0:64, :] = pltpu.roll((q[0:64] & 0xFFFF) | (q[64:128] << 16), by, 1)
    w_ref[64:72, :] = pltpu.roll(jnp.broadcast_to(power.astype(I32), (8, 128)), by, 1)


def encoded_mean(pos, prior, parts):
    return pl.pallas_call(
        mean_kernel,
        in_specs=[SM] + [VM] * 5,
        out_specs=VM,
        out_shape=vmem((72, 128), I32),
        compiler_params=PARAMS,
        name="encoded_mean",
    )(pos, *near(prior, *parts))


def pack_kernel(*refs):
    out = refs[4]
    for i in range(4):
        out[i // 2, (i % 2) * 64 : (i % 2) * 64 + 64, :] = refs[i][0:64, :]
    for c in range(2):
        out[c, 128:136, :] = jnp.where(
            iota((8, 128), 0) == 0, refs[2 * c][64:72, :], refs[2 * c + 1][64:72, :]
        )


def pack(blocks):
    return pl.pallas_call(
        pack_kernel,
        in_specs=[VM] * 4,
        out_specs=VM,
        out_shape=vmem((2, 136, 128), I32),
        compiler_params=PARAMS,
        name="pack",
    )(*near(*blocks))


def spread(pos, pieces, out):
    many = len(pieces)
    arrays = [chunk for piece in pieces for chunk in piece[2]]

    def kernel(pos_ref, *refs):
        ins, (out_ref, made, sems) = refs[: 2 * many], refs[-3:]
        group = iota((64, 128), 1) >> 5
        copies = []
        for p, (colour, d, _) in enumerate(pieces):
            half = pos_ref[1] ^ colour
            first = pos_ref[3 - half]
            lanes = (half * 4 + ((pos_ref[2 + half] + d) & 3)) * 128
            sources = [(group - b - first) & 3 for b in range(4)]
            for q in range(4):
                ref, h = ins[2 * p + q // 2], q % 2
                words = [ref[k, h * 64 : h * 64 + 64, :] for k in range(4)]
                powers = [
                    jnp.broadcast_to(ref[k, 128 + h : 129 + h, :], (8, 128)) for k in range(4)
                ]
                at = p * 4 + q
                for b in range(4):

                    def merge(v, source):
                        v = jnp.where(
                            source < 2,
                            jnp.where(source == 0, v[0], v[1]),
                            jnp.where(source == 2, v[2], v[3]),
                        )
                        return pltpu.roll(v, (128 - 32 * b) % 128, 1) if b else v

                    word = merge(words, sources[b])
                    power = merge(powers, sources[b][0:8]).astype(F32)
                    scale = (jnp.exp2(power) * (1.0 / LEVELS))[0:1]
                    made[at, b, 0:64, :] = ((word << 16) >> 16).astype(F32) * scale
                    made[at, b, 64:128, :] = (word >> 16).astype(F32) * scale
                copy = pltpu.make_async_copy(
                    made.at[at],
                    out_ref.at[:, (pos_ref[0] - q) & 3, :, pl.ds(pl.multiple_of(lanes, 128), 128)],
                    sems.at[at],
                )
                copy.start()
                copies.append(copy)
        for copy in copies:
            copy.wait()

    old = [] if out is None else [out]
    anywhere = pl.BlockSpec(memory_space=pl.ANY)
    return pl.pallas_call(
        kernel,
        in_specs=[SM] + [VM] * (2 * many) + [anywhere] * len(old),
        out_specs=anywhere,
        out_shape=jax.ShapeDtypeStruct((4, 4, 128, 1024), F32),
        scratch_shapes=[
            pltpu.VMEM((4 * many, 4, 128, 128), F32),
            pltpu.SemaphoreType.DMA((4 * many,)),
        ],
        input_output_aliases={1 + 2 * many: 0} if old else {},
        compiler_params=PARAMS,
    )(pos, *near(*arrays), *old)


def shift(v, axis, by):
    size = lax.axis_size(axis)
    return lax.ppermute(v, axis, [(i, (i + by) % size) for i in range(size)])


def turn(v, way, by):
    pairs = []
    for zl in range(2):
        for y in range(4):
            for x in range(4):
                to = (y, (x + by) % 4) if zl == way else ((y + by) % 4, x)
                pairs.append((zl * 16 + y * 4 + x, zl * 16 + to[0] * 4 + to[1]))
    return lax.ppermute(v, ("zl", "y", "x"), pairs)


def ring(v, way):
    opposite = turn(v, way, 2)
    behind, ahead = turn(v, way, 1), turn(v, way, -1)
    return jnp.stack([v, ahead, opposite, behind])


def rings(v, way):
    first, second = v[:, 0], v[:, 1]
    behind0, ahead1 = turn(first, way, 1), turn(second, way, -1)
    behind1, ahead0 = turn(second, way, 1), turn(first, way, -1)
    far0, far1 = turn(behind0, way, 1), turn(ahead1, way, -1)
    return (first, second), (ahead0, ahead1), (far0, far1), (behind0, behind1)


def shards(points, centroids, assign, keep_mask):
    width = points.shape[1]
    swap = [(0, 1), (1, 0)]
    pos = jnp.stack([lax.axis_index(n) for n in ("zh", "zl", "y", "x", "core")]).astype(I32)
    other = lax.ppermute(centroids, "core", swap)

    x = rows_by_columns(points, assign, keep_mask)
    x = lax.all_to_all(x, ("zl", "y", "x"), 0, 0)

    point_f = points.astype(F32)
    point_sq = jnp.sum(point_f * point_f, axis=1)

    cent_f = centroids.astype(F32)
    cent_sq = jnp.sum(cent_f * cent_f, axis=1)
    other_sq = lax.ppermute(cent_sq, "core", swap)

    def nearest(c, c_sq):
        inner = lax.dot_general(points, c, NT, preferred_element_type=F32)
        return jnp.min(c_sq[None, :] - 2.0 * inner, axis=1)

    least = jnp.minimum(nearest(centroids, cent_sq), nearest(other, other_sq))
    row_cost = (point_sq + least) / width
    swapped = jnp.where(pos[1] == 0, pos[2] * 4 + pos[3], 16 + pos[3] * 4 + pos[2])
    slice_at = swapped * 32
    prior = lax.dynamic_slice(
        centroids.reshape(4, 4, 128, width), (0, pos[0], 0, slice_at), (4, 1, 128, 32)
    )
    prior = prior.reshape(4, 128, 32).transpose(1, 0, 2).reshape(128, 128)

    own, send = partial_sums(pos, x, row_cost)
    pieces = add_pieces(own, lax.ppermute(send, "core", swap))
    parts = [pieces[0]] + [shift(pieces[k], "zh", k) for k in range(1, 4)]
    w = encoded_mean(pos, prior, parts)
    opposite = shift(w, "zh", 2)
    mine = pack([w, shift(w, "zh", 1), opposite, shift(w, "zh", 3)])
    theirs = lax.ppermute(mine, "zl", swap)
    colours = rings(ring(mine, 0), 1), rings(ring(theirs, 1), 0)
    both = range(2)
    out = spread(pos, [(c, 0, colours[c][0]) for c in both], None)
    out = spread(pos, [(c, d, colours[c][d]) for c in both for d in (1, 3)], out)
    out = spread(pos, [(c, 2, colours[c][2]) for c in both], out)
    new_centroids = out.reshape(2048, width)
    return new_centroids, row_cost


def solution(mesh):
    grid = Mesh(mesh.devices.reshape(4, 2, 4, 4, 2), ("zh", "zl", "y", "x", "core"))
    rows = ("zh", "zl", "y", "x", "core")
    in_specs = (P(rows, None), P("core", None), P(rows), P(rows))
    out_specs = (P("core", None), P(rows))

    return jax.shard_map(shards, mesh=grid, in_specs=in_specs, out_specs=out_specs, check_vma=False)
```
